32 devices in a mesh: grp: 2 (over y), seq: 4 (over z), head: 2 (over x), batch: 2 (over core).
Axes of the slice: x: 2, y: 2, z: 4, core: 2. Of those that a mesh axis runs over, the one named last changes fastest.
Arguments:
- queries: bfloat16 [64, 64, 128], P(('grp', 'batch'), 'head'), parts along dimension 0, may hold values from -8 to 8
- key_cache: bfloat16 [64, 8, 1024, 128], P(('grp', 'batch'), 'head', 'seq'), parts along dimension 0, may hold values from -5 to 5
- value_cache: bfloat16 [64, 8, 1024, 128], P(('grp', 'batch'), 'head', 'seq'), parts along dimension 0, may hold values from -5 to 5
- gate_logits: float32 [2, 64, 64], P(None, ('grp', 'batch'), 'head'), parts along dimension 1, may hold values from -6 to 6
- lengths: int32 [64], P(('grp', 'batch')), parts along dimension 0, may hold values from 256 to 1024, as said below
- chosen: int32 [64, 8, 2], P(('grp', 'batch'), 'head'), parts along dimension 0, may hold values from 0 to 7, as said below
- counts: int32 [64, 8], P(('grp', 'batch'), 'head'), parts along dimension 0, may hold values from 1 to 2, as said below
Outputs:
- output: bfloat16 [64, 64, 128], P(('grp', 'batch'), 'head'), parts along dimension 0
The draws below stay inside these ranges and needn't reach their ends.
There are 2 independent parts, one for each index of `grp`. The reference program is written for one: setup_inputs(seed, part) draws one part's arguments, and reference() takes and returns one part's arrays. A program takes and returns all parts, laid end to end along the dimension named above; each array names one. Nothing has to cross between parts.
Inputs may be any that keep to these rules, and one draw needn't show every extreme that they name: `lengths`: every draw has a sequence of the full length 1024. `chosen`: for each sequence and key-value head the first counts entries are distinct blocks that start below the sequence's length, and the first entry is block 0; the entries after them are ignored. `counts`: every draw has a sequence with 2 valid entries for every key-value head.
All inputs are finite; a program needn't handle non-finite values.
Results may differ from the reference program's by a relative error of at most 0.02.
Values may be sent and summed in bfloat16 or wider, within the bound.
A program may use at most 64 MiB of HBM per device.

```python
import math
import jax
import jax.numpy as jnp
from jax import lax

D_HEAD = 128
Q_HEADS = 64
KV_HEADS = 8
BLOCK = 128
SEQS = 32
BLOCKS = 8
CTX = 1024
TOPK = 2


def plan_draw(key):
    key_lengths = jax.random.fold_in(key, 11)
    key_scores = jax.random.fold_in(key, 12)
    key_counts = jax.random.fold_in(key, 13)
    key_longest = jax.random.fold_in(key, 14)
    lengths = jax.random.randint(key_lengths, (SEQS,), TOPK * BLOCK, CTX + 1, dtype=jnp.int32)
    longest = jax.random.randint(key_longest, (), 0, SEQS, dtype=jnp.int32)
    seq_ids = jnp.arange(SEQS, dtype=jnp.int32)
    lengths = jnp.where(seq_ids == longest, CTX, lengths).astype(jnp.int32)
    valid_blocks = (lengths + BLOCK - 1) // BLOCK
    block_ids = jnp.arange(BLOCKS, dtype=jnp.int32)
    raw_scores = jax.random.randint(key_scores, (SEQS, KV_HEADS, BLOCKS), 0, 1 << 16, dtype=jnp.int32)
    block_score = raw_scores * BLOCKS + block_ids[None, None, :]
    block_score = jnp.where(block_ids[None, None, :] < valid_blocks[:, None, None], block_score, -1 - block_ids[None, None, :])
    block_score = jnp.where(block_ids[None, None, :] == 0, 1 << 29, block_score)
    chosen = lax.top_k(block_score, TOPK)[1].astype(jnp.int32)
    counts = jax.random.randint(key_counts, (SEQS, KV_HEADS), 1, TOPK + 1, dtype=jnp.int32)
    counts = jnp.where((seq_ids == longest)[:, None], TOPK, counts).astype(jnp.int32)
    return (lengths, chosen, counts)


def draw_lengths(key, part):
    return plan_draw(key)[0]


def draw_chosen(key, part):
    return plan_draw(key)[1]


def draw_counts(key, part):
    return plan_draw(key)[2]


def draw_queries(key, part):
    full_shape = (SEQS, Q_HEADS, D_HEAD)
    drawn = jnp.clip(2.5 * jax.random.normal(jax.random.fold_in(key, 42), full_shape, jnp.float32), -8.0, 8.0)
    return drawn.astype(jnp.bfloat16)


def draw_key_cache(key, part):
    first_shape = (SEQS, KV_HEADS, BLOCK, D_HEAD)
    rest_shape = (SEQS, KV_HEADS, CTX - BLOCK, D_HEAD)
    first_rows = jnp.clip(jax.random.normal(jax.random.fold_in(key, 34), first_shape, jnp.float32), -5.0, 5.0)
    rest_rows = jnp.clip(jax.random.normal(jax.random.fold_in(key, 35), rest_shape, jnp.float32), -5.0, 5.0)
    return jnp.concatenate([first_rows, rest_rows], axis=2).astype(jnp.bfloat16)


def steps_of(key, extent, shards, low, top_value):
    loudness, own = 1.0, jax.random.fold_in(key, 6)
    for dim, blocks in shards:
        draws = jnp.exp(jax.random.uniform(jax.random.fold_in(own, dim), (blocks,), jnp.float32, low / len(shards), top_value / len(shards)))
        loudness = loudness * jnp.repeat(draws, extent[dim] // blocks).reshape([-1 if axis == dim else 1 for axis in range(len(extent))])
    return loudness


def noise(rng, dims, scale, limit, pieces=(), held_as=jnp.bfloat16):
    values = jax.random.normal(rng, dims, jnp.float32) * scale
    if len(pieces) > 0:
        values = steps_of(rng, dims, pieces, -0.22, 0.18) * values
    return jnp.clip(values, min=-limit, max=limit).astype(held_as)


def setup_inputs(seed: int = 0, part: int = 0) -> dict:
    key_list = jax.random.split(jax.random.key(seed), 8)
    part_splits = jax.random.split(jax.random.fold_in(key_list[7], part), 8)
    return {
        "queries": draw_queries(jax.random.fold_in(jax.random.fold_in(key_list[7], part), 71), part),
        "key_cache": draw_key_cache(jax.random.fold_in(jax.random.fold_in(key_list[7], part), 71), part),
        "value_cache": noise(part_splits[2], (SEQS, KV_HEADS, CTX, D_HEAD), 1.0, 5.0, ((0, 2), (1, 2), (2, 4))),
        "gate_logits": noise(part_splits[3], (2, SEQS, Q_HEADS), 1.5, 6.0, ((1, 2), (2, 2)), jnp.float32),
        "lengths": draw_lengths(jax.random.fold_in(jax.random.fold_in(key_list[7], part), 71), part),
        "chosen": draw_chosen(jax.random.fold_in(jax.random.fold_in(key_list[7], part), 71), part),
        "counts": draw_counts(jax.random.fold_in(jax.random.fold_in(key_list[7], part), 71), part),
    }


def attend(query_rows, key_rows, value_rows, live_mask, score_scale):
    scores = jnp.einsum('hgd,hnd->hgn', query_rows, key_rows, precision=lax.Precision.HIGHEST) * score_scale
    scores = jnp.where(live_mask[:, None, :], scores, -1e+30)
    row_max = lax.optimization_barrier(jnp.max(scores, axis=2, keepdims=True))
    weights = jnp.where(live_mask[:, None, :], jnp.exp(scores - row_max), 0.0)
    weight_sum = lax.optimization_barrier(jnp.sum(weights, axis=2, keepdims=True))
    rounded = lax.optimization_barrier(weights.astype(jnp.bfloat16)).astype(jnp.float32)
    summed = jnp.einsum('hgn,hnd->hgd', rounded, value_rows, precision=lax.Precision.HIGHEST)
    return summed / weight_sum

def pool_rows(rows_float, head_count, block_count, head_width, root_fill):
    summed = lax.optimization_barrier(jnp.sum(rows_float.reshape(head_count, block_count, BLOCK, head_width), axis=2)) / root_fill
    return lax.optimization_barrier(summed.astype(jnp.bfloat16)).astype(jnp.float32)

def one_sequence(sequence):
    query_in, key_rows, value_rows, gate_row, length, chosen_row, live_slots = sequence
    head_count, context, head_width = key_rows.shape
    group_size = query_in.shape[0] // head_count
    block_count = context // BLOCK
    score_scale = 1.0 / math.sqrt(head_width)
    query_rows = query_in.reshape(head_count, group_size, head_width).astype(jnp.float32)
    position = jnp.arange(context, dtype=jnp.int32)
    live_mask = position < length
    key_float = jnp.where(live_mask[None, :, None], key_rows.astype(jnp.float32), 0.0)
    value_float = jnp.where(live_mask[None, :, None], value_rows.astype(jnp.float32), 0.0)
    starts = jnp.arange(block_count, dtype=jnp.int32) * BLOCK
    filled = jnp.clip(length - starts, 0, BLOCK)
    root_fill = jnp.sqrt(jnp.maximum(filled, 1).astype(jnp.float32))[None, :, None]
    pooled_keys = pool_rows(key_float, head_count, block_count, head_width, root_fill)
    pooled_values = pool_rows(value_float, head_count, block_count, head_width, root_fill)
    block_live = jnp.broadcast_to((filled > 0)[None, :], (head_count, block_count))
    compressed = attend(query_rows, pooled_keys, pooled_values, block_live, score_scale)
    slot_live = jnp.arange(chosen_row.shape[1], dtype=jnp.int32)[None, :] < live_slots[:, None]
    block_ids = jnp.arange(block_count, dtype=jnp.int32)
    picked = jnp.any((chosen_row[:, :, None] == block_ids[None, None, :]) & slot_live[:, :, None], axis=1)
    token_mask = live_mask[None, :] & jnp.repeat(picked, BLOCK, axis=1)
    selected = attend(query_rows, key_float, value_float, token_mask, score_scale)
    gate_pair = jax.nn.sigmoid(gate_row).reshape(2, head_count, group_size, 1)
    mixed = gate_pair[0] * compressed + gate_pair[1] * selected
    return mixed.reshape(head_count * group_size, head_width).astype(jnp.bfloat16)

def reference(queries, key_cache, value_cache, gate_logits, lengths, chosen, counts):
    gate_rows = jnp.moveaxis(gate_logits, 0, 1)
    return lax.map(one_sequence, (queries, key_cache, value_cache, gate_rows, lengths, chosen, counts))
```

```python
import functools
import math

import jax
import jax.numpy as jnp
from jax import lax
from jax.experimental import pallas as pl
from jax.experimental.pallas import tpu as pltpu
from jax.sharding import PartitionSpec as P

BLOCK = 128
LANES = 128
ROWS = 8
NEG = -1e30
MESH = pl.DeviceIdType.MESH


def kernel(
    n, q_ref, k_hbm, v_hbm, gate_ref, len_ref, chosen_ref, count_ref, o_ref,
    k_buf, v_buf, msg, stat, r_msg, r_stat,
    k_sem, v_sem, ms_sem, mr_sem, ss_sem, sr_sem, gs_sem, gr_sem,
):
    pairs, group, width = q_ref.shape
    tokens = k_hbm.shape[1]
    blocks = tokens // BLOCK
    own = pairs // n
    heads = count_ref.shape[0]
    slots = chosen_ref.shape[1]
    tiles = msg.shape[1] - own
    scale = 1.0 / math.sqrt(width)
    me = lax.axis_index("seq")

    def owner(k):
        return lax.rem(me + 1 + k, n)

    def source(k):
        return lax.rem(me + 2 * n - 1 - k, n)

    def load(k, hbm, buf, sem):
        return pltpu.make_async_copy(hbm.at[pl.ds(owner(k) * own, own)], buf.at[k], sem.at[k])

    for k in range(n):
        load(k, k_hbm, k_buf, k_sem).start()
        load(k, v_hbm, v_buf, v_sem).start()

    barrier = pltpu.get_barrier_semaphore()
    for k in range(n - 1):
        pl.semaphore_signal(barrier, inc=1, device_id={"seq": owner(k)}, device_id_type=MESH)

    lane = lax.broadcasted_iota(jnp.int32, (ROWS, LANES), 1)
    row = lax.broadcasted_iota(jnp.int32, (ROWS, LANES), 0)

    gate_lane = lax.broadcasted_iota(jnp.int32, (ROWS, gate_ref.shape[2]), 1)
    gate_row = lax.broadcasted_iota(jnp.int32, (ROWS, gate_ref.shape[2]), 0)
    gates = []
    for branch in range(2):
        packed = jnp.zeros((ROWS, LANES), jnp.float32)
        for i in range(own):
            p = me * own + i
            b, h = lax.div(p, heads), lax.rem(p, heads)
            logits = jnp.broadcast_to(gate_ref[branch, pl.ds(b, 1), :], gate_lane.shape)
            column = jnp.sum(
                jnp.where(gate_lane == gate_row + h * group, logits, 0.0), axis=1, keepdims=True
            )
            packed = jnp.where(lane == i, column, packed)
        gates.append(jax.nn.sigmoid(packed))

    pl.semaphore_wait(barrier, n - 1)

    def send_msg(k):
        return pltpu.make_async_remote_copy(
            src_ref=msg.at[k], dst_ref=r_msg.at[k], send_sem=ms_sem.at[k], recv_sem=mr_sem.at[k],
            device_id={"seq": owner(k)}, device_id_type=MESH,
        )

    def send_stat(k):
        return pltpu.make_async_remote_copy(
            src_ref=stat.at[k], dst_ref=r_stat.at[k], send_sem=ss_sem.at[k], recv_sem=sr_sem.at[k],
            device_id={"seq": owner(k)}, device_id_type=MESH,
        )

    def part(k, carry):
        target = owner(k)
        load(k, k_hbm, k_buf, k_sem).wait()
        load(k, v_hbm, v_buf, v_sem).wait()
        stats = jnp.zeros((ROWS, LANES), jnp.float32)
        pooled = [jnp.zeros((ROWS, width), jnp.float32)] * tiles
        for i in range(own):
            p = target * own + i
            b, h = lax.div(p, heads), lax.rem(p, heads)
            length = len_ref[b]
            count = count_ref[h, b]
            chosen = [chosen_ref[h, slot, b] for slot in range(slots)]
            scores = lax.dot_general(
                q_ref[p], k_buf[k, i], (((1,), (1,)), ((), ())), preferred_element_type=jnp.float32
            ) * scale
            tile, base = divmod(i * blocks, ROWS)
            masked, chosen_mask, live_rows = [], [], []
            root_rows = jnp.ones((ROWS, LANES), jnp.float32)
            for j in range(blocks):
                block = me * blocks + j
                filled = jnp.clip(length - block * BLOCK, 0, BLOCK)
                limit = jnp.int32(0)
                for slot in range(slots):
                    hit = jnp.logical_and(chosen[slot] == block, slot < count)
                    limit = jnp.where(hit, filled, limit)
                part_scores = scores[:, j * BLOCK : (j + 1) * BLOCK]
                live = lane < filled
                inside = lane < limit
                filled_rows = jnp.full((ROWS, LANES), filled, jnp.int32)
                root = lax.rsqrt(jnp.maximum(filled_rows, 1).astype(jnp.float32))
                total = jnp.sum(jnp.where(live, part_scores, 0.0), axis=1, keepdims=True)
                pooled_score = jnp.where(filled_rows > 0, total * root, NEG)
                stats = jnp.where(lane == (1 + j) * own + i, pooled_score, stats)
                root_rows = jnp.where(row == base + j, root, root_rows)
                live_rows.append(jnp.where(jnp.logical_and(live, row == base + j), 1.0, 0.0))
                chosen_mask.append(inside)
                masked.append(jnp.where(inside, part_scores, NEG))
            top = functools.reduce(jnp.maximum, masked)
            top = jnp.max(top, axis=1, keepdims=True)
            weights = [
                jnp.where(inside, jnp.exp(m - top), 0.0) for inside, m in zip(chosen_mask, masked)
            ]
            weight_sum = jnp.sum(functools.reduce(jnp.add, weights), axis=1, keepdims=True)
            safe_sum = jnp.maximum(weight_sum, 1.0)
            log_sum = jnp.where(weight_sum > 0.0, top + jnp.log(safe_sum), NEG)
            stats = jnp.where(lane == i, log_sum, stats)
            left = jnp.concatenate(
                [jnp.concatenate(weights, axis=1), jnp.concatenate(live_rows, axis=1)], axis=0
            ).astype(jnp.bfloat16)
            summed = jnp.dot(left, v_buf[k, i], preferred_element_type=jnp.float32)
            msg[k, i] = (summed[:ROWS] / safe_sum).astype(jnp.bfloat16)
            pooled[tile] = pooled[tile] + summed[ROWS:] * root_rows
        for tile in range(tiles):
            msg[k, own + tile] = pooled[tile].astype(jnp.bfloat16)
        stat[k] = stats

        @pl.when(k < n - 1)
        def _():
            send_stat(k).start()
            send_msg(k).start()

        return carry

    lax.fori_loop(0, n, part, 0)

    for k in range(n - 1):
        send_stat(k).wait_recv()
    all_stats = [r_stat[k] for k in range(n - 1)] + [stat[n - 1]]
    top = functools.reduce(jnp.maximum, all_stats)
    shares = [jnp.exp(s - top) for s in all_stats]
    factor = gates[1] / functools.reduce(jnp.add, shares)
    shares = [s * factor for s in shares]
    block_scores = [
        [pltpu.roll(s, LANES - (1 + j) * own, 1) for j in range(blocks)] for s in all_stats
    ]
    flat = [s for per_device in block_scores for s in per_device]
    top = functools.reduce(jnp.maximum, flat)
    block_shares = [[jnp.exp(s - top) for s in per_device] for per_device in block_scores]
    flat = [s for per_device in block_shares for s in per_device]
    factor = gates[0] / functools.reduce(jnp.add, flat)
    block_shares = [[s * factor for s in per_device] for per_device in block_shares]

    for k in range(n - 1):
        send_msg(k).wait_recv()
    for tile in range(tiles):
        tile_rows = [r_msg[k, own + tile].astype(jnp.float32) for k in range(n - 1)]
        tile_rows.append(msg[n - 1, own + tile].astype(jnp.float32))
        for i in range(own):
            if (i * blocks) // ROWS != tile:
                continue
            base = (i * blocks) % ROWS
            total = jnp.zeros((ROWS, width), jnp.float32)
            for k in range(n):
                partial = msg[k, i] if k == n - 1 else r_msg[k, i]
                total += shares[k][:, i : i + 1] * partial.astype(jnp.float32)
                for j in range(blocks):
                    total += (
                        block_shares[k][j][:, i : i + 1] * tile_rows[k][base + j : base + j + 1, :]
                    )
            o_ref[me * own + i] = total.astype(jnp.bfloat16)

    def share(k, holder):
        rows = o_ref.at[pl.ds(holder * own, own)]
        return pltpu.make_async_remote_copy(
            src_ref=rows, dst_ref=rows, send_sem=gs_sem.at[k], recv_sem=gr_sem.at[k],
            device_id={"seq": owner(k)}, device_id_type=MESH,
        )

    for k in range(n - 1):
        share(k, me).start()
    for k in range(n - 1):
        send_stat(k).wait_send()
        send_msg(k).wait_send()
    for k in range(n - 1):
        share(k, source(k)).wait_recv()
    for k in range(n - 1):
        share(k, me).wait_send()


def on_device(n, queries, key_cache, value_cache, gate_logits, lengths, chosen, counts):
    batch_rows, head_count, context, width = key_cache.shape
    pairs = batch_rows * head_count
    group = queries.shape[1] // head_count
    blocks = context // BLOCK
    own = pairs // n
    tiles = -(-own * blocks // ROWS)
    assert pairs % n == 0 and group == ROWS and ROWS % blocks == 0
    assert own * (1 + blocks) <= LANES
    vmem = pl.BlockSpec(memory_space=pltpu.VMEM)
    smem = pl.BlockSpec(memory_space=pltpu.SMEM)
    hbm = pl.BlockSpec(memory_space=pl.ANY)
    dma = pltpu.SemaphoreType.DMA((n,))
    output = pl.pallas_call(
        functools.partial(kernel, n),
        out_shape=jax.ShapeDtypeStruct((pairs, group, width), jnp.bfloat16),
        in_specs=[vmem, hbm, hbm, vmem, smem, smem, smem],
        out_specs=vmem,
        scratch_shapes=[
            pltpu.VMEM((n, own, context, width), jnp.bfloat16),
            pltpu.VMEM((n, own, context, width), jnp.bfloat16),
            pltpu.VMEM((n, own + tiles, group, width), jnp.bfloat16),
            pltpu.VMEM((n, ROWS, LANES), jnp.float32),
            pltpu.VMEM((n, own + tiles, group, width), jnp.bfloat16),
            pltpu.VMEM((n, ROWS, LANES), jnp.float32),
        ] + [dma] * 8,
        compiler_params=pltpu.CompilerParams(collective_id=0, has_side_effects=True),
    )(
        queries.reshape(pairs, group, width),
        key_cache.reshape(pairs, context, width),
        value_cache.reshape(pairs, context, width),
        gate_logits,
        lengths,
        chosen.transpose(1, 2, 0),
        counts.transpose(1, 0),
    )
    return output.reshape(batch_rows, head_count * group, width)


def solution(mesh):
    return jax.shard_map(
        functools.partial(on_device, mesh.shape["seq"]),
        mesh=mesh,
        in_specs=(
            P(("grp", "batch"), "head", None),
            P(("grp", "batch"), "head", "seq", None),
            P(("grp", "batch"), "head", "seq", None),
            P(None, ("grp", "batch"), "head"),
            P(("grp", "batch")),
            P(("grp", "batch"), "head", None),
            P(("grp", "batch"), "head"),
        ),
        out_specs=P(("grp", "batch"), "head", None),
        check_vma=False,
    )
```

```python
import functools
import math

import jax
import jax.numpy as jnp
from jax import lax
from jax.experimental import pallas as pl
from jax.experimental.pallas import tpu as pltpu
from jax.sharding import PartitionSpec as P

BLOCK = 128
LANES = 128
ROWS = 8
NEG = -1e30
MESH = pl.DeviceIdType.MESH


def kernel(
    n, q_ref, k_hbm, v_hbm, gate_ref, len_ref, chosen_ref, count_ref, o_ref,
    k_buf, v_buf, msg, stat, r_msg, r_stat,
    k_sem, v_sem, ms_sem, mr_sem, ss_sem, sr_sem, gs_sem, gr_sem,
):
    pairs, group, width = q_ref.shape
    tokens = k_hbm.shape[1]
    blocks = tokens // BLOCK
    own = pairs // n
    heads = count_ref.shape[0]
    slots = chosen_ref.shape[1]
    tiles = msg.shape[1] - own
    scale = 1.0 / math.sqrt(width)
    me = lax.axis_index("seq")

    def owner(k):
        return lax.rem(me + 1 + k, n)

    def source(k):
        return lax.rem(me + 2 * n - 1 - k, n)

    def load(k, hbm, buf, sem):
        return pltpu.make_async_copy(hbm.at[pl.ds(owner(k) * own, own)], buf.at[k], sem.at[k])

    for k in range(n):
        load(k, k_hbm, k_buf, k_sem).start()
        load(k, v_hbm, v_buf, v_sem).start()

    barrier = pltpu.get_barrier_semaphore()
    for k in range(n - 1):
        pl.semaphore_signal(barrier, inc=1, device_id={"seq": owner(k)}, device_id_type=MESH)

    lane = lax.broadcasted_iota(jnp.int32, (ROWS, LANES), 1)
    row = lax.broadcasted_iota(jnp.int32, (ROWS, LANES), 0)

    lane_pair = lax.div(lane, group)

    def gate_row(branch):
        if own % heads == 0:
            first = me * (own // heads)
            pieces = [gate_ref[branch, pl.ds(first + r, 1), :] for r in range(own // heads)]
        else:
            first = me * own
            line = gate_ref[branch, pl.ds(lax.div(first, heads), 1), :]
            picked = line[:, : own * group]
            for o in range(1, heads // own):
                here = lax.rem(first, heads) == o * own
                picked = jnp.where(here, line[:, o * own * group : (o + 1) * own * group], picked)
            pieces = [picked]
        if own * group < LANES:
            pieces.append(jnp.zeros((1, LANES - own * group), jnp.float32))
        return jax.nn.sigmoid(jnp.concatenate(pieces, axis=1))

    gates = jnp.where(row == 0, gate_row(1), gate_row(0))
    token = lax.broadcasted_iota(jnp.int32, (BLOCK, LANES), 0)

    pl.semaphore_wait(barrier, n - 1)

    def send_msg(k):
        return pltpu.make_async_remote_copy(
            src_ref=msg.at[k], dst_ref=r_msg.at[k], send_sem=ms_sem.at[k], recv_sem=mr_sem.at[k],
            device_id={"seq": owner(k)}, device_id_type=MESH,
        )

    def send_stat(k):
        return pltpu.make_async_remote_copy(
            src_ref=stat.at[k], dst_ref=r_stat.at[k], send_sem=ss_sem.at[k], recv_sem=sr_sem.at[k],
            device_id={"seq": owner(k)}, device_id_type=MESH,
        )

    def part(k, carry):
        target = owner(k)
        first = target * own
        lengths = [len_ref[lax.div(first + i, heads)] for i in range(own)]

        def spread(values):
            line = jnp.full((1, LANES), values[0], jnp.int32)
            for i in range(1, own):
                line = jnp.where(lane_pair[:1] == i, values[i], line)
            return line

        length_line = spread(lengths)
        pair_ids = [(lax.rem(first + i, heads), lax.div(first + i, heads)) for i in range(own)]
        count_line = spread([count_ref[h, b] for h, b in pair_ids])
        chosen_lines = [spread([chosen_ref[h, slot, b] for h, b in pair_ids]) for slot in range(slots)]
        chosen_lines = [jnp.where(slot < count_line, line, -1) for slot, line in enumerate(chosen_lines)]

        rows = q_ref[pl.ds(first, own)].astype(jnp.float32).reshape(own * group, width)
        if own * group < LANES:
            rows = jnp.concatenate([rows, jnp.zeros((LANES - own * group, width), jnp.float32)], axis=0)
        columns = rows.T
        load(k, k_hbm, k_buf, k_sem).wait()
        scores = None
        for i in range(0, own, 2):
            both = range(i, min(i + 2, own))
            held = jnp.concatenate(
                [jnp.where(lane_pair[:1] == p, columns, 0.0) for p in both], axis=0
            ).astype(jnp.bfloat16)
            keys = jnp.concatenate([k_buf[k, p] for p in both], axis=1)
            product = jnp.dot(keys, held, preferred_element_type=jnp.float32)
            scores = product if scores is None else scores + product
        scores = scores * scale

        stats = jnp.zeros((ROWS, LANES), jnp.float32)
        masked, inside = [], []
        for j in range(blocks):
            block = me * blocks + j
            filled = jnp.clip(length_line - block * BLOCK, 0, BLOCK)
            hits = [line == block for line in chosen_lines]
            limit = jnp.where(functools.reduce(jnp.logical_or, hits), filled, 0)
            block_scores = scores[j * BLOCK : (j + 1) * BLOCK]
            root = lax.rsqrt(jnp.maximum(filled, 1).astype(jnp.float32))
            total = jnp.sum(jnp.where(token < filled, block_scores, 0.0), axis=0, keepdims=True)
            stats = jnp.where(row == 1 + j, jnp.where(filled > 0, total * root, NEG), stats)
            inside.append(token < limit)
            masked.append(jnp.where(inside[j], block_scores, NEG))
        top = jnp.max(functools.reduce(jnp.maximum, masked), axis=0, keepdims=True)
        weights = [jnp.where(i, jnp.exp(m - top), 0.0) for i, m in zip(inside, masked)]
        weight_sum = jnp.sum(functools.reduce(jnp.add, weights), axis=0, keepdims=True)
        safe_sum = jnp.maximum(weight_sum, 1.0)
        log_sum = jnp.where(weight_sum > 0.0, top + jnp.log(safe_sum), NEG)
        stats = jnp.where(row == 0, log_sum, stats)
        stat[k] = stats
        inverse = 1.0 / safe_sum
        weight_rows = jnp.concatenate([(w * inverse).T for w in weights], axis=1)

        load(k, v_hbm, v_buf, v_sem).wait()
        per_tile = ROWS // blocks
        for tile in range(tiles):
            members = range(tile * per_tile, min((tile + 1) * per_tile, own))
            length_rows = jnp.zeros((ROWS, LANES), jnp.int32)
            for at, i in enumerate(members):
                length_rows = jnp.where(lax.div(row, blocks) == at, lengths[i], length_rows)
            start_rows = (me * blocks + lax.rem(row, blocks)) * BLOCK
            filled_rows = jnp.clip(length_rows - start_rows, 0, BLOCK)
            root_rows = lax.rsqrt(jnp.maximum(filled_rows, 1).astype(jnp.float32))
            live = lane < filled_rows
            pooled = jnp.zeros((ROWS, width), jnp.float32)
            for at, i in enumerate(members):
                live_rows = jnp.concatenate(
                    [jnp.where(live & (row == at * blocks + j), 1.0, 0.0) for j in range(blocks)], axis=1
                )
                left = jnp.concatenate([weight_rows[i * group : (i + 1) * group], live_rows], axis=0)
                summed = jnp.dot(
                    left.astype(jnp.bfloat16), v_buf[k, i], preferred_element_type=jnp.float32
                )
                msg[k, i] = summed[:group].astype(jnp.bfloat16)
                pooled = pooled + summed[group:]
            msg[k, own + tile] = (pooled * root_rows).astype(jnp.bfloat16)

        @pl.when(k < n - 1)
        def _():
            send_stat(k).start()
            send_msg(k).start()

        return carry

    lax.fori_loop(0, n, part, 0)

    for k in range(n - 1):
        send_stat(k).wait_recv()
    all_stats = [r_stat[k] for k in range(n - 1)] + [stat[n - 1]]
    top = functools.reduce(jnp.maximum, all_stats)
    block_row = (row >= 1) & (row <= blocks)
    block_top = jnp.max(jnp.where(block_row, top, NEG), axis=0, keepdims=True)
    top = jnp.where(row == 0, top, block_top)
    shares = [jnp.where(row <= blocks, jnp.exp(s - top), 0.0) for s in all_stats]
    total = functools.reduce(jnp.add, shares)
    block_total = jnp.sum(jnp.where(block_row, total, 0.0), axis=0, keepdims=True)
    factor = gates / jnp.where(row == 0, total, block_total)
    shares = [s * factor for s in shares]
    per_turn = LANES // ROWS
    turned = []
    for k in range(0, n, per_turn):
        stack = shares[k : k + per_turn]
        if len(stack) < per_turn:
            stack.append(jnp.zeros((LANES - len(stack) * ROWS, LANES), jnp.float32))
        turned.append(jnp.concatenate(stack, axis=0).T)

    def coefficient(k, i, which):
        at = (k % per_turn) * ROWS + which
        return turned[k // per_turn][i * group : (i + 1) * group, at : at + 1]

    for k in range(n - 1):
        send_msg(k).wait_recv()
    for tile in range(tiles):
        tile_rows = [r_msg[k, own + tile].astype(jnp.float32) for k in range(n - 1)]
        tile_rows.append(msg[n - 1, own + tile].astype(jnp.float32))
        for i in range(own):
            if (i * blocks) // ROWS != tile:
                continue
            base = (i * blocks) % ROWS
            total = jnp.zeros((ROWS, width), jnp.float32)
            for k in range(n):
                partial = msg[k, i] if k == n - 1 else r_msg[k, i]
                total += coefficient(k, i, 0) * partial.astype(jnp.float32)
                for j in range(blocks):
                    total += coefficient(k, i, 1 + j) * tile_rows[k][base + j : base + j + 1, :]
            o_ref[me * own + i] = total.astype(jnp.bfloat16)

    def share(k, holder):
        rows = o_ref.at[pl.ds(holder * own, own)]
        return pltpu.make_async_remote_copy(
            src_ref=rows, dst_ref=rows, send_sem=gs_sem.at[k], recv_sem=gr_sem.at[k],
            device_id={"seq": owner(k)}, device_id_type=MESH,
        )

    for k in range(n - 1):
        share(k, me).start()
    for k in range(n - 1):
        send_stat(k).wait_send()
        send_msg(k).wait_send()
    for k in range(n - 1):
        share(k, source(k)).wait_recv()
    for k in range(n - 1):
        share(k, me).wait_send()


def on_device(n, queries, key_cache, value_cache, gate_logits, lengths, chosen, counts):
    batch_rows, head_count, context, width = key_cache.shape
    pairs = batch_rows * head_count
    group = queries.shape[1] // head_count
    blocks = context // BLOCK
    own = pairs // n
    tiles = -(-own * blocks // ROWS)
    assert pairs % n == 0 and group == ROWS and ROWS % blocks == 0
    assert own * group <= LANES and 1 + blocks <= ROWS and width == LANES
    vmem = pl.BlockSpec(memory_space=pltpu.VMEM)
    smem = pl.BlockSpec(memory_space=pltpu.SMEM)
    hbm = pl.BlockSpec(memory_space=pl.ANY)
    dma = pltpu.SemaphoreType.DMA((n,))
    output = pl.pallas_call(
        functools.partial(kernel, n),
        out_shape=jax.ShapeDtypeStruct((pairs, group, width), jnp.bfloat16),
        in_specs=[vmem, hbm, hbm, vmem, smem, smem, smem],
        out_specs=vmem,
        scratch_shapes=[
            pltpu.VMEM((n, own, context, width), jnp.bfloat16),
            pltpu.VMEM((n, own, context, width), jnp.bfloat16),
            pltpu.VMEM((n, own + tiles, group, width), jnp.bfloat16),
            pltpu.VMEM((n, ROWS, LANES), jnp.float32),
            pltpu.VMEM((n, own + tiles, group, width), jnp.bfloat16),
            pltpu.VMEM((n, ROWS, LANES), jnp.float32),
        ] + [dma] * 8,
        compiler_params=pltpu.CompilerParams(collective_id=0, has_side_effects=True),
    )(
        queries.reshape(pairs, group, width),
        key_cache.reshape(pairs, context, width),
        value_cache.reshape(pairs, context, width),
        gate_logits,
        lengths,
        chosen.transpose(1, 2, 0),
        counts.transpose(1, 0),
    )
    return output.reshape(batch_rows, head_count * group, width)


def solution(mesh):
    return jax.shard_map(
        functools.partial(on_device, mesh.shape["seq"]),
        mesh=mesh,
        in_specs=(
            P(("grp", "batch"), "head", None),
            P(("grp", "batch"), "head", "seq", None),
            P(("grp", "batch"), "head", "seq", None),
            P(None, ("grp", "batch"), "head"),
            P(("grp", "batch")),
            P(("grp", "batch"), "head", None),
            P(("grp", "batch"), "head"),
        ),
        out_specs=P(("grp", "batch"), "head", None),
        check_vma=False,
    )
```

```python
import functools
import math

import jax
import jax.numpy as jnp
from jax import lax
from jax.experimental import pallas as pl
from jax.experimental.pallas import tpu as pltpu
from jax.sharding import PartitionSpec as P

BLOCK = 128
LANES = 128
ROWS = 8
NEG = -1e30
MESH = pl.DeviceIdType.MESH


def kernel(
    n, q_ref, k_hbm, v_hbm, gate_ref, len_ref, chosen_ref, count_ref, o_ref,
    k_buf, v_buf, msg, stat, r_msg, r_stat,
    k_sem, v_sem, ms_sem, mr_sem, ss_sem, sr_sem, gs_sem, gr_sem,
):
    pairs, group, width = q_ref.shape
    tokens = k_hbm.shape[1]
    blocks = tokens // BLOCK
    own = pairs // n
    heads = count_ref.shape[0]
    slots = chosen_ref.shape[1]
    tiles = msg.shape[1] - own
    scale = 1.0 / math.sqrt(width)
    me = lax.axis_index("seq")

    def owner(k):
        return lax.rem(me + 1 + k, n)

    def source(k):
        return lax.rem(me + 2 * n - 1 - k, n)

    def load(k, hbm, buf, sem):
        return pltpu.make_async_copy(hbm.at[pl.ds(owner(k) * own, own)], buf.at[k], sem.at[k])

    for k in range(n):
        load(k, k_hbm, k_buf, k_sem).start()
        load(k, v_hbm, v_buf, v_sem).start()

    barrier = pltpu.get_barrier_semaphore()
    for k in range(n - 1):
        pl.semaphore_signal(barrier, inc=1, device_id={"seq": owner(k)}, device_id_type=MESH)

    lane = lax.broadcasted_iota(jnp.int32, (ROWS, LANES), 1)
    row = lax.broadcasted_iota(jnp.int32, (ROWS, LANES), 0)

    lane_pair = lax.div(lane, group)

    def gate_row(branch):
        if own % heads == 0:
            first = me * (own // heads)
            pieces = [gate_ref[branch, pl.ds(first + r, 1), :] for r in range(own // heads)]
        else:
            first = me * own
            line = gate_ref[branch, pl.ds(lax.div(first, heads), 1), :]
            picked = line[:, : own * group]
            for o in range(1, heads // own):
                here = lax.rem(first, heads) == o * own
                picked = jnp.where(here, line[:, o * own * group : (o + 1) * own * group], picked)
            pieces = [picked]
        if own * group < LANES:
            pieces.append(jnp.zeros((1, LANES - own * group), jnp.float32))
        return jax.nn.sigmoid(jnp.concatenate(pieces, axis=1))

    gates = jnp.where(row == 0, gate_row(1), gate_row(0))
    token = lax.broadcasted_iota(jnp.int32, (BLOCK, LANES), 0)

    def send_msg(k):
        return pltpu.make_async_remote_copy(
            src_ref=msg.at[k], dst_ref=r_msg.at[k], send_sem=ms_sem.at[k], recv_sem=mr_sem.at[k],
            device_id={"seq": owner(k)}, device_id_type=MESH,
        )

    def send_stat(k):
        return pltpu.make_async_remote_copy(
            src_ref=stat.at[k], dst_ref=r_stat.at[k], send_sem=ss_sem.at[k], recv_sem=sr_sem.at[k],
            device_id={"seq": owner(k)}, device_id_type=MESH,
        )

    def part(k, carry):
        target = owner(k)
        first = target * own
        lengths = [len_ref[lax.div(first + i, heads)] for i in range(own)]

        def spread(values):
            line = jnp.full((1, LANES), values[0], jnp.int32)
            for i in range(1, own):
                line = jnp.where(lane_pair[:1] == i, values[i], line)
            return line

        length_line = spread(lengths)
        pair_ids = [(lax.rem(first + i, heads), lax.div(first + i, heads)) for i in range(own)]
        count_line = spread([count_ref[h, b] for h, b in pair_ids])
        chosen_lines = [spread([chosen_ref[h, slot, b] for h, b in pair_ids]) for slot in range(slots)]
        chosen_lines = [jnp.where(slot < count_line, line, -1) for slot, line in enumerate(chosen_lines)]

        rows = q_ref[pl.ds(first, own)].astype(jnp.float32).reshape(own * group, width)
        if own * group < LANES:
            rows = jnp.concatenate([rows, jnp.zeros((LANES - own * group, width), jnp.float32)], axis=0)
        columns = rows.T
        load(k, k_hbm, k_buf, k_sem).wait()
        scores = None
        for i in range(0, own, 2):
            both = range(i, min(i + 2, own))
            held = jnp.concatenate(
                [jnp.where(lane_pair[:1] == p, columns, 0.0) for p in both], axis=0
            ).astype(jnp.bfloat16)
            keys = jnp.concatenate([k_buf[k, p] for p in both], axis=1)
            product = jnp.dot(keys, held, preferred_element_type=jnp.float32)
            scores = product if scores is None else scores + product
        scores = scores * scale

        stats = jnp.zeros((ROWS, LANES), jnp.float32)
        masked, inside = [], []
        for j in range(blocks):
            block = me * blocks + j
            filled = jnp.clip(length_line - block * BLOCK, 0, BLOCK)
            hits = [line == block for line in chosen_lines]
            limit = jnp.where(functools.reduce(jnp.logical_or, hits), filled, 0)
            block_scores = scores[j * BLOCK : (j + 1) * BLOCK]
            root = lax.rsqrt(jnp.maximum(filled, 1).astype(jnp.float32))
            total = jnp.sum(jnp.where(token < filled, block_scores, 0.0), axis=0, keepdims=True)
            stats = jnp.where(row == 1 + j, jnp.where(filled > 0, total * root, NEG), stats)
            inside.append(token < limit)
            masked.append(jnp.where(inside[j], block_scores, NEG))
        top = jnp.max(functools.reduce(jnp.maximum, masked), axis=0, keepdims=True)
        weights = [jnp.where(i, jnp.exp(m - top), 0.0) for i, m in zip(inside, masked)]
        weight_sum = jnp.sum(functools.reduce(jnp.add, weights), axis=0, keepdims=True)
        safe_sum = jnp.maximum(weight_sum, 1.0)
        log_sum = jnp.where(weight_sum > 0.0, top + jnp.log(safe_sum), NEG)
        stats = jnp.where(row == 0, log_sum, stats)
        stat[k] = stats
        inverse = 1.0 / safe_sum
        weight_rows = jnp.concatenate([(w * inverse).T for w in weights], axis=1)

        load(k, v_hbm, v_buf, v_sem).wait()
        per_tile = ROWS // blocks
        for tile in range(tiles):
            members = range(tile * per_tile, min((tile + 1) * per_tile, own))
            length_rows = jnp.zeros((ROWS, LANES), jnp.int32)
            for at, i in enumerate(members):
                length_rows = jnp.where(lax.div(row, blocks) == at, lengths[i], length_rows)
            start_rows = (me * blocks + lax.rem(row, blocks)) * BLOCK
            filled_rows = jnp.clip(length_rows - start_rows, 0, BLOCK)
            root_rows = lax.rsqrt(jnp.maximum(filled_rows, 1).astype(jnp.float32))
            live = lane < filled_rows
            pooled = jnp.zeros((ROWS, width), jnp.float32)
            for at, i in enumerate(members):
                live_rows = jnp.concatenate(
                    [jnp.where(live & (row == at * blocks + j), 1.0, 0.0) for j in range(blocks)], axis=1
                )
                left = jnp.concatenate([weight_rows[i * group : (i + 1) * group], live_rows], axis=0)
                summed = jnp.dot(
                    left.astype(jnp.bfloat16), v_buf[k, i], preferred_element_type=jnp.float32
                )
                msg[k, i] = summed[:group].astype(jnp.bfloat16)
                pooled = pooled + summed[group:]
            msg[k, own + tile] = (pooled * root_rows).astype(jnp.bfloat16)

        @pl.when(k == 0)
        def _():
            pl.semaphore_wait(barrier, n - 1)

        @pl.when(k < n - 1)
        def _():
            send_stat(k).start()
            send_msg(k).start()

        return carry

    lax.fori_loop(0, n, part, 0)

    for k in range(n - 1):
        send_stat(k).wait_recv()
    all_stats = [r_stat[k] for k in range(n - 1)] + [stat[n - 1]]
    top = functools.reduce(jnp.maximum, all_stats)
    block_row = (row >= 1) & (row <= blocks)
    block_top = jnp.max(jnp.where(block_row, top, NEG), axis=0, keepdims=True)
    top = jnp.where(row == 0, top, block_top)
    shares = [jnp.where(row <= blocks, jnp.exp(s - top), 0.0) for s in all_stats]
    total = functools.reduce(jnp.add, shares)
    block_total = jnp.sum(jnp.where(block_row, total, 0.0), axis=0, keepdims=True)
    factor = gates / jnp.where(row == 0, total, block_total)
    shares = [s * factor for s in shares]
    per_turn = LANES // ROWS
    turned = []
    for k in range(0, n, per_turn):
        stack = shares[k : k + per_turn]
        if len(stack) < per_turn:
            stack.append(jnp.zeros((LANES - len(stack) * ROWS, LANES), jnp.float32))
        turned.append(jnp.concatenate(stack, axis=0).T)

    def coefficient(k, i, which):
        at = (k % per_turn) * ROWS + which
        return turned[k // per_turn][i * group : (i + 1) * group, at : at + 1]

    for k in range(n - 1):
        send_msg(k).wait_recv()
    for tile in range(tiles):
        tile_rows = [r_msg[k, own + tile].astype(jnp.float32) for k in range(n - 1)]
        tile_rows.append(msg[n - 1, own + tile].astype(jnp.float32))
        for i in range(own):
            if (i * blocks) // ROWS != tile:
                continue
            base = (i * blocks) % ROWS
            total = jnp.zeros((ROWS, width), jnp.float32)
            for k in range(n):
                partial = msg[k, i] if k == n - 1 else r_msg[k, i]
                total += coefficient(k, i, 0) * partial.astype(jnp.float32)
                for j in range(blocks):
                    total += coefficient(k, i, 1 + j) * tile_rows[k][base + j : base + j + 1, :]
            o_ref[me * own + i] = total.astype(jnp.bfloat16)

    def share(k, holder):
        rows = o_ref.at[pl.ds(holder * own, own)]
        return pltpu.make_async_remote_copy(
            src_ref=rows, dst_ref=rows, send_sem=gs_sem.at[k], recv_sem=gr_sem.at[k],
            device_id={"seq": owner(k)}, device_id_type=MESH,
        )

    for k in range(n - 1):
        share(k, me).start()
    for k in range(n - 1):
        send_stat(k).wait_send()
        send_msg(k).wait_send()
    for k in range(n - 1):
        share(k, source(k)).wait_recv()
    for k in range(n - 1):
        share(k, me).wait_send()


def on_device(n, queries, key_cache, value_cache, gate_logits, lengths, chosen, counts):
    batch_rows, head_count, context, width = key_cache.shape
    pairs = batch_rows * head_count
    group = queries.shape[1] // head_count
    blocks = context // BLOCK
    own = pairs // n
    tiles = -(-own * blocks // ROWS)
    assert pairs % n == 0 and group == ROWS and ROWS % blocks == 0
    assert own * group <= LANES and 1 + blocks <= ROWS and width == LANES
    vmem = pl.BlockSpec(memory_space=pltpu.VMEM)
    smem = pl.BlockSpec(memory_space=pltpu.SMEM)
    hbm = pl.BlockSpec(memory_space=pl.ANY)
    dma = pltpu.SemaphoreType.DMA((n,))
    output = pl.pallas_call(
        functools.partial(kernel, n),
        out_shape=pltpu.VMEM((pairs, group, width), jnp.bfloat16),
        in_specs=[vmem, hbm, hbm, vmem, smem, smem, smem],
        out_specs=vmem,
        scratch_shapes=[
            pltpu.VMEM((n, own, context, width), jnp.bfloat16),
            pltpu.VMEM((n, own, context, width), jnp.bfloat16),
            pltpu.VMEM((n, own + tiles, group, width), jnp.bfloat16),
            pltpu.VMEM((n, ROWS, LANES), jnp.float32),
            pltpu.VMEM((n, own + tiles, group, width), jnp.bfloat16),
            pltpu.VMEM((n, ROWS, LANES), jnp.float32),
        ] + [dma] * 8,
        compiler_params=pltpu.CompilerParams(collective_id=0, has_side_effects=True),
    )(
        queries.reshape(pairs, group, width),
        key_cache.reshape(pairs, context, width),
        value_cache.reshape(pairs, context, width),
        gate_logits,
        lengths,
        chosen.transpose(1, 2, 0),
        counts.transpose(1, 0),
    )
    return output.reshape(batch_rows, head_count * group, width)


def solution(mesh):
    return jax.shard_map(
        functools.partial(on_device, mesh.shape["seq"]),
        mesh=mesh,
        in_specs=(
            P(("grp", "batch"), "head", None),
            P(("grp", "batch"), "head", "seq", None),
            P(("grp", "batch"), "head", "seq", None),
            P(None, ("grp", "batch"), "head"),
            P(("grp", "batch")),
            P(("grp", "batch"), "head", None),
            P(("grp", "batch"), "head"),
        ),
        out_specs=P(("grp", "batch"), "head", None),
        check_vma=False,
    )
```

```python
import functools
import math

import jax
import jax.numpy as jnp
from jax import lax
from jax.experimental import pallas as pl
from jax.experimental.pallas import tpu as pltpu
from jax.sharding import PartitionSpec as P

BLOCK = 128
LANES = 128
ROWS = 8
NEG = -1e30
MESH = pl.DeviceIdType.MESH


def kernel(
    n, q_ref, k_hbm, v_hbm, gate_ref, len_ref, chosen_ref, count_ref, o_ref,
    k_buf, v_buf, msg, stat, r_msg, r_stat,
    k_sem, v_sem, ms_sem, mr_sem, ss_sem, sr_sem, gs_sem, gr_sem,
):
    pairs, group, width = q_ref.shape
    tokens = k_hbm.shape[1]
    blocks = tokens // BLOCK
    own = pairs // n
    heads = count_ref.shape[0]
    slots = chosen_ref.shape[1]
    tiles = msg.shape[1] - own
    scale = 1.0 / math.sqrt(width)
    me = lax.axis_index("seq")

    holders = n // 2
    turns = n // holders
    low = (n - holders) // 2

    far = jnp.where(me < n // 2, (holders + 1) // 2, 0)

    def chunk_at(k):
        return lax.rem(lax.rem(k, holders) + far, holders) * turns + lax.div(k, holders)

    def owner(c):
        return low + lax.div(c, turns)

    def peer(r):
        return lax.rem(me + r, n)

    def load(k, hbm, buf, sem):
        return pltpu.make_async_copy(hbm.at[pl.ds(chunk_at(k) * own, own)], buf.at[k], sem.at[k])

    for k in range(n):
        load(k, k_hbm, k_buf, k_sem).start()
        load(k, v_hbm, v_buf, v_sem).start()

    barrier = pltpu.get_barrier_semaphore()
    for r in range(1, n):
        pl.semaphore_signal(barrier, inc=1, device_id={"seq": peer(r)}, device_id_type=MESH)

    lane = lax.broadcasted_iota(jnp.int32, (ROWS, LANES), 1)
    row = lax.broadcasted_iota(jnp.int32, (ROWS, LANES), 0)

    lane_pair = lax.div(lane, group)

    def gate_row(branch, first_pair):
        if own % heads == 0:
            first = lax.div(first_pair, heads)
            pieces = [gate_ref[branch, pl.ds(first + r, 1), :] for r in range(own // heads)]
        else:
            first = first_pair
            line = gate_ref[branch, pl.ds(lax.div(first, heads), 1), :]
            picked = line[:, : own * group]
            for o in range(1, heads // own):
                here = lax.rem(first, heads) == o * own
                picked = jnp.where(here, line[:, o * own * group : (o + 1) * own * group], picked)
            pieces = [picked]
        if own * group < LANES:
            pieces.append(jnp.zeros((1, LANES - own * group), jnp.float32))
        return jax.nn.sigmoid(jnp.concatenate(pieces, axis=1))

    token = lax.broadcasted_iota(jnp.int32, (BLOCK, LANES), 0)

    def send(k, held, landed, send_sem, recv_sem):
        c = chunk_at(k)
        turn = lax.rem(c, turns)
        slot = lax.rem(me - owner(c) + n, n) - 1
        return pltpu.make_async_remote_copy(
            src_ref=held.at[k], dst_ref=landed.at[turn, slot],
            send_sem=send_sem.at[k], recv_sem=recv_sem.at[turn, slot],
            device_id={"seq": owner(c)}, device_id_type=MESH,
        )

    def arrival(turn, slot, held, landed, send_sem, recv_sem):
        return pltpu.make_async_remote_copy(
            src_ref=held.at[0], dst_ref=landed.at[turn, slot],
            send_sem=send_sem.at[0], recv_sem=recv_sem.at[turn, slot],
            device_id={"seq": peer(1 + slot)}, device_id_type=MESH,
        )

    stat_path = (stat, r_stat, ss_sem, sr_sem)
    msg_path = (msg, r_msg, ms_sem, mr_sem)

    def part(k, carry):
        target = chunk_at(k)
        first = target * own
        lengths = [len_ref[lax.div(first + i, heads)] for i in range(own)]

        def spread(values):
            line = jnp.full((1, LANES), values[0], jnp.int32)
            for i in range(1, own):
                line = jnp.where(lane_pair[:1] == i, values[i], line)
            return line

        length_line = spread(lengths)
        pair_ids = [(lax.rem(first + i, heads), lax.div(first + i, heads)) for i in range(own)]
        count_line = spread([count_ref[h, b] for h, b in pair_ids])
        chosen_lines = [spread([chosen_ref[h, slot, b] for h, b in pair_ids]) for slot in range(slots)]
        chosen_lines = [jnp.where(slot < count_line, line, -1) for slot, line in enumerate(chosen_lines)]

        rows = q_ref[pl.ds(first, own)].astype(jnp.float32).reshape(own * group, width)
        if own * group < LANES:
            rows = jnp.concatenate([rows, jnp.zeros((LANES - own * group, width), jnp.float32)], axis=0)
        columns = rows.T
        load(k, k_hbm, k_buf, k_sem).wait()
        scores = None
        for i in range(0, own, 2):
            both = range(i, min(i + 2, own))
            held = jnp.concatenate(
                [jnp.where(lane_pair[:1] == p, columns, 0.0) for p in both], axis=0
            ).astype(jnp.bfloat16)
            keys = jnp.concatenate([k_buf[k, p] for p in both], axis=1)
            product = jnp.dot(keys, held, preferred_element_type=jnp.float32)
            scores = product if scores is None else scores + product
        scores = scores * scale

        stats = jnp.zeros((ROWS, LANES), jnp.float32)
        masked, inside = [], []
        for j in range(blocks):
            block = me * blocks + j
            filled = jnp.clip(length_line - block * BLOCK, 0, BLOCK)
            hits = [line == block for line in chosen_lines]
            limit = jnp.where(functools.reduce(jnp.logical_or, hits), filled, 0)
            block_scores = scores[j * BLOCK : (j + 1) * BLOCK]
            root = lax.rsqrt(jnp.maximum(filled, 1).astype(jnp.float32))
            total = jnp.sum(jnp.where(token < filled, block_scores, 0.0), axis=0, keepdims=True)
            stats = jnp.where(row == 1 + j, jnp.where(filled > 0, total * root, NEG), stats)
            inside.append(token < limit)
            masked.append(jnp.where(inside[j], block_scores, NEG))
        top = jnp.max(functools.reduce(jnp.maximum, masked), axis=0, keepdims=True)
        weights = [jnp.where(i, jnp.exp(m - top), 0.0) for i, m in zip(inside, masked)]
        weight_sum = jnp.sum(functools.reduce(jnp.add, weights), axis=0, keepdims=True)
        safe_sum = jnp.maximum(weight_sum, 1.0)
        log_sum = jnp.where(weight_sum > 0.0, top + jnp.log(safe_sum), NEG)
        stats = jnp.where(row == 0, log_sum, stats)
        stat[k] = stats
        inverse = 1.0 / safe_sum
        weight_rows = jnp.concatenate([(w * inverse).T for w in weights], axis=1)

        load(k, v_hbm, v_buf, v_sem).wait()
        per_tile = ROWS // blocks
        for tile in range(tiles):
            members = range(tile * per_tile, min((tile + 1) * per_tile, own))
            length_rows = jnp.zeros((ROWS, LANES), jnp.int32)
            for at, i in enumerate(members):
                length_rows = jnp.where(lax.div(row, blocks) == at, lengths[i], length_rows)
            start_rows = (me * blocks + lax.rem(row, blocks)) * BLOCK
            filled_rows = jnp.clip(length_rows - start_rows, 0, BLOCK)
            root_rows = lax.rsqrt(jnp.maximum(filled_rows, 1).astype(jnp.float32))
            live = lane < filled_rows
            pooled = jnp.zeros((ROWS, width), jnp.float32)
            for at, i in enumerate(members):
                live_rows = jnp.concatenate(
                    [jnp.where(live & (row == at * blocks + j), 1.0, 0.0) for j in range(blocks)], axis=1
                )
                left = jnp.concatenate([weight_rows[i * group : (i + 1) * group], live_rows], axis=0)
                summed = jnp.dot(
                    left.astype(jnp.bfloat16), v_buf[k, i], preferred_element_type=jnp.float32
                )
                msg[k, i] = summed[:group].astype(jnp.bfloat16)
                pooled = pooled + summed[group:]
            msg[k, own + tile] = (pooled * root_rows).astype(jnp.bfloat16)

        @pl.when(k == 0)
        def _():
            pl.semaphore_wait(barrier, n - 1)

        @pl.when(owner(target) != me)
        def _():
            send(k, *stat_path).start()
            send(k, *msg_path).start()

        return carry

    lax.fori_loop(0, n, part, 0)

    def share(turn, r):
        c = (me - low) * turns + turn
        rows = o_ref.at[pl.ds(c * own, own)]
        return pltpu.make_async_remote_copy(
            src_ref=rows, dst_ref=rows, send_sem=gs_sem.at[turn, r - 1], recv_sem=gr_sem.at[c],
            device_id={"seq": peer(r)}, device_id_type=MESH,
        )

    def finish(turn):
        c = (me - low) * turns + turn
        home = turn * holders + lax.rem(me - low + holders - far, holders)
        gates = jnp.where(row == 0, gate_row(1, c * own), gate_row(0, c * own))
        for slot in range(n - 1):
            arrival(turn, slot, *stat_path).wait_recv()
        all_stats = [r_stat[turn, slot] for slot in range(n - 1)] + [stat[home]]
        top = functools.reduce(jnp.maximum, all_stats)
        block_row = (row >= 1) & (row <= blocks)
        block_top = jnp.max(jnp.where(block_row, top, NEG), axis=0, keepdims=True)
        top = jnp.where(row == 0, top, block_top)
        shares = [jnp.where(row <= blocks, jnp.exp(s - top), 0.0) for s in all_stats]
        total = functools.reduce(jnp.add, shares)
        block_total = jnp.sum(jnp.where(block_row, total, 0.0), axis=0, keepdims=True)
        factor = gates / jnp.where(row == 0, total, block_total)
        shares = [s * factor for s in shares]
        per_turn = LANES // ROWS
        turned = []
        for k in range(0, n, per_turn):
            stack = shares[k : k + per_turn]
            if len(stack) < per_turn:
                stack.append(jnp.zeros((LANES - len(stack) * ROWS, LANES), jnp.float32))
            turned.append(jnp.concatenate(stack, axis=0).T)

        def coefficient(k, i, which):
            at = (k % per_turn) * ROWS + which
            return turned[k // per_turn][i * group : (i + 1) * group, at : at + 1]

        for slot in range(n - 1):
            arrival(turn, slot, *msg_path).wait_recv()
        for tile in range(tiles):
            tile_rows = [r_msg[turn, slot, own + tile].astype(jnp.float32) for slot in range(n - 1)]
            tile_rows.append(msg[home, own + tile].astype(jnp.float32))
            for i in range(own):
                if (i * blocks) // ROWS != tile:
                    continue
                base = (i * blocks) % ROWS
                total = jnp.zeros((ROWS, width), jnp.float32)
                for k in range(n):
                    partial = msg[home, i] if k == n - 1 else r_msg[turn, k, i]
                    total += coefficient(k, i, 0) * partial.astype(jnp.float32)
                    for j in range(blocks):
                        total += coefficient(k, i, 1 + j) * tile_rows[k][base + j : base + j + 1, :]
                o_ref[c * own + i] = total.astype(jnp.bfloat16)
        for r in range(1, n):
            share(turn, r).start()

    holds = jnp.logical_and(me >= low, me < low + holders)

    @pl.when(holds)
    def _():
        for turn in range(turns):
            finish(turn)

    def drain(k, carry):
        @pl.when(owner(chunk_at(k)) != me)
        def _():
            send(k, *stat_path).wait_send()
            send(k, *msg_path).wait_send()

        return carry

    def collect(c, carry):
        @pl.when(owner(c) != me)
        def _():
            rows = o_ref.at[pl.ds(c * own, own)]
            pltpu.make_async_remote_copy(
                src_ref=rows, dst_ref=rows, send_sem=gs_sem.at[0, 0], recv_sem=gr_sem.at[c],
                device_id={"seq": owner(c)}, device_id_type=MESH,
            ).wait_recv()

        return carry

    lax.fori_loop(0, n, drain, 0)
    lax.fori_loop(0, n, collect, 0)

    @pl.when(holds)
    def _():
        for turn in range(turns):
            for r in range(1, n):
                share(turn, r).wait_send()


def on_device(n, queries, key_cache, value_cache, gate_logits, lengths, chosen, counts):
    batch_rows, head_count, context, width = key_cache.shape
    pairs = batch_rows * head_count
    group = queries.shape[1] // head_count
    blocks = context // BLOCK
    own = pairs // n
    tiles = -(-own * blocks // ROWS)
    assert n % 2 == 0 and pairs % n == 0 and group == ROWS and ROWS % blocks == 0
    assert own * group <= LANES and 1 + blocks <= ROWS and width == LANES
    vmem = pl.BlockSpec(memory_space=pltpu.VMEM)
    smem = pl.BlockSpec(memory_space=pltpu.SMEM)
    hbm = pl.BlockSpec(memory_space=pl.ANY)
    turns = n // (n // 2)
    dma = pltpu.SemaphoreType.DMA((n,))
    dma2 = pltpu.SemaphoreType.DMA((turns, n - 1))
    output = pl.pallas_call(
        functools.partial(kernel, n),
        out_shape=pltpu.VMEM((pairs, group, width), jnp.bfloat16),
        in_specs=[vmem, hbm, hbm, vmem, smem, smem, smem],
        out_specs=vmem,
        scratch_shapes=[
            pltpu.VMEM((n, own, context, width), jnp.bfloat16),
            pltpu.VMEM((n, own, context, width), jnp.bfloat16),
            pltpu.VMEM((n, own + tiles, group, width), jnp.bfloat16),
            pltpu.VMEM((n, ROWS, LANES), jnp.float32),
            pltpu.VMEM((turns, n - 1, own + tiles, group, width), jnp.bfloat16),
            pltpu.VMEM((turns, n - 1, ROWS, LANES), jnp.float32),
            dma, dma, dma, dma2, dma, dma2, dma2, dma,
        ],
        compiler_params=pltpu.CompilerParams(collective_id=0, has_side_effects=True),
    )(
        queries.reshape(pairs, group, width),
        key_cache.reshape(pairs, context, width),
        value_cache.reshape(pairs, context, width),
        gate_logits,
        lengths,
        chosen.transpose(1, 2, 0),
        counts.transpose(1, 0),
    )
    return output.reshape(batch_rows, head_count * group, width)


def solution(mesh):
    return jax.shard_map(
        functools.partial(on_device, mesh.shape["seq"]),
        mesh=mesh,
        in_specs=(
            P(("grp", "batch"), "head", None),
            P(("grp", "batch"), "head", "seq", None),
            P(("grp", "batch"), "head", "seq", None),
            P(None, ("grp", "batch"), "head"),
            P(("grp", "batch")),
            P(("grp", "batch"), "head", None),
            P(("grp", "batch"), "head"),
        ),
        out_specs=P(("grp", "batch"), "head", None),
        check_vma=False,
    )
```

```python
import functools
import math

import jax
import jax.numpy as jnp
from jax import lax
from jax.experimental import pallas as pl
from jax.experimental.pallas import tpu as pltpu
from jax.sharding import PartitionSpec as P

BLOCK = 128
LANES = 128
ROWS = 8
NEG = -1e30
MESH = pl.DeviceIdType.MESH


def kernel(
    n, q_ref, k_hbm, v_hbm, gate_ref, len_ref, chosen_ref, count_ref, o_ref,
    k_buf, v_buf, msg, stat, r_msg, r_stat,
    k_sem, v_sem, ms_sem, mr_sem, ss_sem, sr_sem, gs_sem, gr_sem,
):
    pairs, group, width = q_ref.shape
    tokens = k_hbm.shape[1]
    blocks = tokens // BLOCK
    own = pairs // n
    heads = count_ref.shape[0]
    slots = chosen_ref.shape[1]
    tiles = msg.shape[1] - own
    scale = 1.0 / math.sqrt(width)
    me = lax.axis_index("seq")

    holders = n // 2
    turns = n // holders
    low = (n - holders) // 2

    far = jnp.where(me < n // 2, (holders + 1) // 2, 0)

    def chunk_at(k):
        return lax.rem(lax.rem(k, holders) + far, holders) * turns + lax.div(k, holders)

    def owner(c):
        return low + lax.div(c, turns)

    def peer(r):
        return lax.rem(me + r, n)

    def load(k, hbm, buf, sem):
        return pltpu.make_async_copy(hbm.at[pl.ds(chunk_at(k) * own, own)], buf.at[k], sem.at[k])

    for k in range(n):
        load(k, k_hbm, k_buf, k_sem).start()
        load(k, v_hbm, v_buf, v_sem).start()

    barrier = pltpu.get_barrier_semaphore()
    holds = jnp.logical_and(me >= low, me < low + holders)
    for r in range(1, n):
        other = peer(r)

        @pl.when(jnp.logical_or(holds, jnp.logical_and(other >= low, other < low + holders)))
        def _(other=other):
            pl.semaphore_signal(barrier, inc=1, device_id={"seq": other}, device_id_type=MESH)

    lane = lax.broadcasted_iota(jnp.int32, (ROWS, LANES), 1)
    row = lax.broadcasted_iota(jnp.int32, (ROWS, LANES), 0)

    lane_pair = lax.div(lane, group)

    def gate_row(branch, first_pair):
        if own % heads == 0:
            first = lax.div(first_pair, heads)
            pieces = [gate_ref[branch, pl.ds(first + r, 1), :] for r in range(own // heads)]
        else:
            first = first_pair
            line = gate_ref[branch, pl.ds(lax.div(first, heads), 1), :]
            picked = line[:, : own * group]
            for o in range(1, heads // own):
                here = lax.rem(first, heads) == o * own
                picked = jnp.where(here, line[:, o * own * group : (o + 1) * own * group], picked)
            pieces = [picked]
        if own * group < LANES:
            pieces.append(jnp.zeros((1, LANES - own * group), jnp.float32))
        return jax.nn.sigmoid(jnp.concatenate(pieces, axis=1))

    all_gates = []
    for turn in range(turns):
        gate_pair = lax.rem((me - low) * turns + turn + n, n) * own
        all_gates.append(jnp.where(row == 0, gate_row(1, gate_pair), gate_row(0, gate_pair)))
    token = lax.broadcasted_iota(jnp.int32, (BLOCK, LANES), 0)

    def send(k, held, landed, send_sem, recv_sem):
        c = chunk_at(k)
        turn = lax.rem(c, turns)
        slot = lax.rem(me - owner(c) + n, n) - 1
        return pltpu.make_async_remote_copy(
            src_ref=held.at[k], dst_ref=landed.at[turn, slot],
            send_sem=send_sem.at[k], recv_sem=recv_sem.at[turn, slot],
            device_id={"seq": owner(c)}, device_id_type=MESH,
        )

    def arrival(turn, slot, held, landed, send_sem, recv_sem):
        return pltpu.make_async_remote_copy(
            src_ref=held.at[0], dst_ref=landed.at[turn, slot],
            send_sem=send_sem.at[0], recv_sem=recv_sem.at[turn, slot],
            device_id={"seq": peer(1 + slot)}, device_id_type=MESH,
        )

    stat_path = (stat, r_stat, ss_sem, sr_sem)
    msg_path = (msg, r_msg, ms_sem, mr_sem)

    def part(k, carry):
        target = chunk_at(k)
        first = target * own
        lengths = [len_ref[lax.div(first + i, heads)] for i in range(own)]

        def spread(values):
            line = jnp.full((1, LANES), values[0], jnp.int32)
            for i in range(1, own):
                line = jnp.where(lane_pair[:1] == i, values[i], line)
            return line

        length_line = spread(lengths)
        pair_ids = [(lax.rem(first + i, heads), lax.div(first + i, heads)) for i in range(own)]
        count_line = spread([count_ref[h, b] for h, b in pair_ids])
        chosen_lines = [spread([chosen_ref[h, slot, b] for h, b in pair_ids]) for slot in range(slots)]
        chosen_lines = [jnp.where(slot < count_line, line, -1) for slot, line in enumerate(chosen_lines)]

        rows = q_ref[pl.ds(first, own)].astype(jnp.float32).reshape(own * group, width)
        if own * group < LANES:
            rows = jnp.concatenate([rows, jnp.zeros((LANES - own * group, width), jnp.float32)], axis=0)
        columns = rows.T
        load(k, k_hbm, k_buf, k_sem).wait()
        scores = None
        for i in range(0, own, 2):
            both = range(i, min(i + 2, own))
            held = jnp.concatenate(
                [jnp.where(lane_pair[:1] == p, columns, 0.0) for p in both], axis=0
            ).astype(jnp.bfloat16)
            keys = jnp.concatenate([k_buf[k, p] for p in both], axis=1)
            product = jnp.dot(keys, held, preferred_element_type=jnp.float32)
            scores = product if scores is None else scores + product
        scores = scores * scale

        stats = jnp.zeros((ROWS, LANES), jnp.float32)
        masked, inside = [], []
        for j in range(blocks):
            block = me * blocks + j
            filled = jnp.clip(length_line - block * BLOCK, 0, BLOCK)
            hits = [line == block for line in chosen_lines]
            limit = jnp.where(functools.reduce(jnp.logical_or, hits), filled, 0)
            block_scores = scores[j * BLOCK : (j + 1) * BLOCK]
            root = lax.rsqrt(jnp.maximum(filled, 1).astype(jnp.float32))
            total = jnp.sum(jnp.where(token < filled, block_scores, 0.0), axis=0, keepdims=True)
            stats = jnp.where(row == 1 + j, jnp.where(filled > 0, total * root, NEG), stats)
            inside.append(token < limit)
            masked.append(jnp.where(inside[j], block_scores, NEG))
        top = jnp.max(functools.reduce(jnp.maximum, masked), axis=0, keepdims=True)
        weights = [jnp.where(i, jnp.exp(m - top), 0.0) for i, m in zip(inside, masked)]
        weight_sum = jnp.sum(functools.reduce(jnp.add, weights), axis=0, keepdims=True)
        safe_sum = jnp.maximum(weight_sum, 1.0)
        log_sum = jnp.where(weight_sum > 0.0, top + jnp.log(safe_sum), NEG)
        stats = jnp.where(row == 0, log_sum, stats)
        stat[k] = stats
        inverse = 1.0 / safe_sum
        weight_rows = jnp.concatenate([(w * inverse).T for w in weights], axis=1)

        load(k, v_hbm, v_buf, v_sem).wait()
        per_tile = ROWS // blocks
        for tile in range(tiles):
            members = range(tile * per_tile, min((tile + 1) * per_tile, own))
            length_rows = jnp.zeros((ROWS, LANES), jnp.int32)
            for at, i in enumerate(members):
                length_rows = jnp.where(lax.div(row, blocks) == at, lengths[i], length_rows)
            start_rows = (me * blocks + lax.rem(row, blocks)) * BLOCK
            filled_rows = jnp.clip(length_rows - start_rows, 0, BLOCK)
            root_rows = lax.rsqrt(jnp.maximum(filled_rows, 1).astype(jnp.float32))
            live = lane < filled_rows
            pooled = jnp.zeros((ROWS, width), jnp.float32)
            for at, i in enumerate(members):
                live_rows = jnp.concatenate(
                    [jnp.where(live & (row == at * blocks + j), 1.0, 0.0) for j in range(blocks)], axis=1
                )
                left = jnp.concatenate([weight_rows[i * group : (i + 1) * group], live_rows], axis=0)
                summed = jnp.dot(
                    left.astype(jnp.bfloat16), v_buf[k, i], preferred_element_type=jnp.float32
                )
                msg[k, i] = summed[:group].astype(jnp.bfloat16)
                pooled = pooled + summed[group:]
            msg[k, own + tile] = (pooled * root_rows).astype(jnp.bfloat16)

        @pl.when(k == 0)
        def _():
            pl.semaphore_wait(barrier, jnp.where(holds, n - 1, holders))

        @pl.when(owner(target) != me)
        def _():
            send(k, *stat_path).start()
            send(k, *msg_path).start()

        return carry

    lax.fori_loop(0, n, part, 0, unroll=4)

    def share(turn, r):
        c = (me - low) * turns + turn
        rows = o_ref.at[pl.ds(c * own, own)]
        return pltpu.make_async_remote_copy(
            src_ref=rows, dst_ref=rows, send_sem=gs_sem.at[turn, r - 1], recv_sem=gr_sem.at[c],
            device_id={"seq": peer(r)}, device_id_type=MESH,
        )

    def finish(turn):
        c = (me - low) * turns + turn
        home = turn * holders + lax.rem(me - low + holders - far, holders)
        gates = all_gates[turn]
        for slot in range(n - 1):
            arrival(turn, slot, *stat_path).wait_recv()
        all_stats = [r_stat[turn, slot] for slot in range(n - 1)] + [stat[home]]
        top = functools.reduce(jnp.maximum, all_stats)
        block_row = (row >= 1) & (row <= blocks)
        block_top = jnp.max(jnp.where(block_row, top, NEG), axis=0, keepdims=True)
        top = jnp.where(row == 0, top, block_top)
        shares = [jnp.where(row <= blocks, jnp.exp(s - top), 0.0) for s in all_stats]
        total = functools.reduce(jnp.add, shares)
        block_total = jnp.sum(jnp.where(block_row, total, 0.0), axis=0, keepdims=True)
        factor = gates / jnp.where(row == 0, total, block_total)
        shares = [s * factor for s in shares]
        per_turn = LANES // ROWS
        turned = []
        for k in range(0, n, per_turn):
            stack = shares[k : k + per_turn]
            if len(stack) < per_turn:
                stack.append(jnp.zeros((LANES - len(stack) * ROWS, LANES), jnp.float32))
            turned.append(jnp.concatenate(stack, axis=0).T)

        def coefficient(k, i, which):
            at = (k % per_turn) * ROWS + which
            return turned[k // per_turn][i * group : (i + 1) * group, at : at + 1]

        for slot in range(n - 1):
            arrival(turn, slot, *msg_path).wait_recv()
        for tile in range(tiles):
            tile_rows = [r_msg[turn, slot, own + tile].astype(jnp.float32) for slot in range(n - 1)]
            tile_rows.append(msg[home, own + tile].astype(jnp.float32))
            for i in range(own):
                if (i * blocks) // ROWS != tile:
                    continue
                base = (i * blocks) % ROWS
                total = jnp.zeros((ROWS, width), jnp.float32)
                for k in range(n):
                    partial = msg[home, i] if k == n - 1 else r_msg[turn, k, i]
                    total += coefficient(k, i, 0) * partial.astype(jnp.float32)
                    for j in range(blocks):
                        total += coefficient(k, i, 1 + j) * tile_rows[k][base + j : base + j + 1, :]
                o_ref[c * own + i] = total.astype(jnp.bfloat16)
        for r in range(1, n):
            share(turn, r).start()

    @pl.when(holds)
    def _():
        for turn in range(turns):
            finish(turn)

    def drain(k, carry):
        @pl.when(owner(chunk_at(k)) != me)
        def _():
            send(k, *stat_path).wait_send()
            send(k, *msg_path).wait_send()

        return carry

    def collect(c, carry):
        @pl.when(owner(c) != me)
        def _():
            rows = o_ref.at[pl.ds(c * own, own)]
            pltpu.make_async_remote_copy(
                src_ref=rows, dst_ref=rows, send_sem=gs_sem.at[0, 0], recv_sem=gr_sem.at[c],
                device_id={"seq": owner(c)}, device_id_type=MESH,
            ).wait_recv()

        return carry

    lax.fori_loop(0, n, drain, 0)
    lax.fori_loop(0, n, collect, 0)

    @pl.when(holds)
    def _():
        for turn in range(turns):
            for r in range(1, n):
                share(turn, r).wait_send()


def on_device(n, queries, key_cache, value_cache, gate_logits, lengths, chosen, counts):
    batch_rows, head_count, context, width = key_cache.shape
    pairs = batch_rows * head_count
    group = queries.shape[1] // head_count
    blocks = context // BLOCK
    own = pairs // n
    tiles = -(-own * blocks // ROWS)
    assert n % 2 == 0 and pairs % n == 0 and group == ROWS and ROWS % blocks == 0
    assert own * group <= LANES and 1 + blocks <= ROWS and width == LANES
    vmem = pl.BlockSpec(memory_space=pltpu.VMEM)
    smem = pl.BlockSpec(memory_space=pltpu.SMEM)
    hbm = pl.BlockSpec(memory_space=pl.ANY)
    turns = n // (n // 2)
    dma = pltpu.SemaphoreType.DMA((n,))
    dma2 = pltpu.SemaphoreType.DMA((turns, n - 1))
    output = pl.pallas_call(
        functools.partial(kernel, n),
        out_shape=pltpu.VMEM((pairs, group, width), jnp.bfloat16),
        in_specs=[vmem, hbm, hbm, vmem, smem, smem, smem],
        out_specs=vmem,
        scratch_shapes=[
            pltpu.VMEM((n, own, context, width), jnp.bfloat16),
            pltpu.VMEM((n, own, context, width), jnp.bfloat16),
            pltpu.VMEM((n, own + tiles, group, width), jnp.bfloat16),
            pltpu.VMEM((n, ROWS, LANES), jnp.float32),
            pltpu.VMEM((turns, n - 1, own + tiles, group, width), jnp.bfloat16),
            pltpu.VMEM((turns, n - 1, ROWS, LANES), jnp.float32),
            dma, dma, dma, dma2, dma, dma2, dma2, dma,
        ],
        compiler_params=pltpu.CompilerParams(collective_id=0, has_side_effects=True),
    )(
        queries.reshape(pairs, group, width),
        key_cache.reshape(pairs, context, width),
        value_cache.reshape(pairs, context, width),
        gate_logits,
        lengths,
        chosen.transpose(1, 2, 0),
        counts.transpose(1, 0),
    )
    return output.reshape(batch_rows, head_count * group, width)


def solution(mesh):
    return jax.shard_map(
        functools.partial(on_device, mesh.shape["seq"]),
        mesh=mesh,
        in_specs=(
            P(("grp", "batch"), "head", None),
            P(("grp", "batch"), "head", "seq", None),
            P(("grp", "batch"), "head", "seq", None),
            P(None, ("grp", "batch"), "head"),
            P(("grp", "batch")),
            P(("grp", "batch"), "head", None),
            P(("grp", "batch"), "head"),
        ),
        out_specs=P(("grp", "batch"), "head", None),
        check_vma=False,
    )
```
